32 devices in a mesh: freq: 8 (over y, x, core), feed: 4 (over z).
Axes of the slice: x: 2, y: 2, z: 4, core: 2. Of those that a mesh axis runs over, the one named last changes fastest.
Arguments:
- voltages: int32 [32, 2048, 2, 768], P(None, ('feed', 'freq')), may hold values from -127 to 127
- gains: float32 [2, 32, 2048], P(None, None, ('feed', 'freq')), may hold values from -0.06 to 0.06
Outputs:
- visibilities: float32 [32, 2, 2048, 2048], P('freq', None, 'feed')
The draws below stay inside these ranges and needn't reach their ends.
All inputs are finite; a program needn't handle non-finite values.
Results may differ from the reference program's by a relative error of at most 0.0031.
Values may be sent and summed in bfloat16 or wider, within the bound.
No kernel may reach another device: no remote copies, remote signals or barrier semaphores. Data moves between devices by JAX's collectives and lax.ppermute only.
A program may use at most 192 MiB of HBM per device.

```python
import jax
import jax.numpy as jnp
from jax import lax

FEEDS = 2048
TIME = 768
CHAN = 32


def set_ends(array, rng, low, top_value):
    place = [jax.random.randint(jax.random.fold_in(rng, axis), (), 0, length) for axis, length in enumerate(array.shape)]
    longest = array.shape.index(max(array.shape))
    beside = place[:longest] + [(place[longest] + 1) % array.shape[longest]] + place[longest + 1:]
    return array.at[tuple(place)].set(low).at[tuple(beside)].set(top_value)


def block_scale(rng, dims, shards, least, top_value):
    loudness = 1.0
    for position, blocks in shards:
        draws = jax.random.uniform(jax.random.fold_in(jax.random.fold_in(rng, 6), position), (blocks,), jnp.float32, least / len(shards), top_value / len(shards))
        loudness = loudness * jnp.repeat(jnp.exp(draws), dims[position] // blocks).reshape((-1,) + (1,) * (len(dims) - 1 - position))
    return loudness


def gaussian(rng, dims, scale, limit, cuts=(), held_as=jnp.bfloat16):
    values = scale * jax.random.normal(rng, dims, jnp.float32)
    if cuts:
        values = values * block_scale(rng, dims, cuts, -0.22, 0.18)
    return jnp.clip(values, -limit, limit).astype(held_as)


def setup_inputs(seed: int = 0) -> dict:
    key_list = jax.random.split(jax.random.key(seed), 3)
    voltages = set_ends(jax.random.randint(key_list[0], (CHAN, FEEDS, 2, TIME), -127, 128), jax.random.fold_in(key_list[0], 1), -127, 127).astype(jnp.int32)
    gains = gaussian(key_list[1], (2, CHAN, FEEDS), 0.01, 0.06, ((2, 32),), jnp.float32)
    return {"voltages": voltages, "gains": gains}


def reference(voltages, gains):
    volt_real = voltages[:, :, 0, :].astype(jnp.float32)
    volt_imag = voltages[:, :, 1, :].astype(jnp.float32)
    gain_real = gains[0][:, :, None]
    gain_imag = gains[1][:, :, None]
    eq_real = gain_real * volt_real - gain_imag * volt_imag
    eq_imag = gain_real * volt_imag + gain_imag * volt_real
    equalized = jnp.stack([eq_real, eq_imag], axis=2).astype(jnp.bfloat16)

    def per_channel(block):
        columns = block.reshape(FEEDS, 2 * TIME)
        swapped = jnp.concatenate([block[:, 1, :], -block[:, 0, :]], axis=1)
        left_side = jnp.concatenate([columns, swapped], axis=0)
        result = jnp.dot(left_side, columns.T, preferred_element_type=jnp.float32)
        return result.reshape(2, FEEDS, FEEDS) * (1.0 / TIME)

    return lax.map(per_channel, equalized)
```

```python
import functools

import jax
import jax.numpy as jnp
from jax import lax
from jax.experimental import pallas as pl
from jax.experimental.pallas import tpu as pltpu
from jax.sharding import PartitionSpec as P

CONTRACT_LAST = (((1,), (1,)), ((), ()))
INWARD = ((0, 1), (3, 2))
MIDDLE = ((1, 2), (2, 1))
OUTWARD = ((1, 0), (2, 3))


def equalize_kernel(volt_ref, gain_ref, out_ref):
    samples = volt_ref.shape[-1]
    gain_real = gain_ref[0, :, 0:1]
    gain_imag = gain_ref[0, :, 1:2]
    volt_real = volt_ref[0, :, 0, :].astype(jnp.float32)
    volt_imag = volt_ref[0, :, 1, :].astype(jnp.float32)
    out_ref[0, :, :samples] = (gain_real * volt_real - gain_imag * volt_imag).astype(jnp.bfloat16)
    out_ref[0, :, samples:] = (gain_real * volt_imag + gain_imag * volt_real).astype(jnp.bfloat16)


def equalize(voltages, gains, chunk, freq_count):
    channels, feeds, _, samples = voltages.shape
    owned = channels // freq_count
    return pl.pallas_call(
        equalize_kernel,
        grid=(freq_count,),
        in_specs=[
            pl.BlockSpec((1, feeds, 2, samples), lambda f: (f * owned + chunk, 0, 0, 0)),
            pl.BlockSpec((1, feeds, 2), lambda f: (f * owned + chunk, 0, 0)),
        ],
        out_specs=pl.BlockSpec((1, feeds, 2 * samples), lambda f: (f, 0, 0)),
        out_shape=jax.ShapeDtypeStruct((freq_count, feeds, 2 * samples), jnp.bfloat16),
        cost_estimate=pl.CostEstimate(
            flops=6 * freq_count * feeds * samples * 2,
            bytes_accessed=freq_count * feeds * samples * 12,
            transcendentals=0,
        ),
        name="equalize",
    )(voltages, gains)


def visibility(left, right, samples):
    turned = jnp.concatenate([-right[:, samples:], right[:, :samples]], axis=1)
    real_part = lax.dot_general(left, right, CONTRACT_LAST, preferred_element_type=jnp.float32)
    imag_part = lax.dot_general(left, turned, CONTRACT_LAST, preferred_element_type=jnp.float32)
    return real_part * (1.0 / samples), imag_part * (1.0 / samples)


def own_kernel(place_ref, own_ref, other_ref, *refs):
    out_ref = refs[-1]
    samples = own_ref.shape[1] // 2
    real_part, imag_part = visibility(own_ref[...], other_ref[...], samples)
    out_ref[0, 0] = real_part
    out_ref[0, 1] = imag_part


def own_block(out, out_shape, chunk, place, own, other, name):
    rows, depth = own.shape
    half = rows // 2
    in_specs = [
        pl.BlockSpec((rows, depth), lambda j, p: (0, 0)),
        pl.BlockSpec((half, depth), lambda j, p: (j, 0)),
    ]
    operands = [own, other]
    aliases = {}
    if out is not None:
        in_specs.append(pl.BlockSpec(memory_space=pl.ANY))
        operands.append(out)
        aliases = {3: 0}
    return pl.pallas_call(
        own_kernel,
        grid_spec=pltpu.PrefetchScalarGridSpec(
            num_scalar_prefetch=1,
            grid=(2,),
            in_specs=in_specs,
            out_specs=pl.BlockSpec((1, 2, rows, half), lambda j, p: (chunk, 0, 0, p[0] * 2 + j)),
        ),
        out_shape=out_shape,
        input_output_aliases=aliases,
        cost_estimate=pl.CostEstimate(
            flops=4 * rows * rows * depth, bytes_accessed=4 * rows * depth + 8 * rows * rows, transcendentals=0
        ),
        name=name,
    )(place, *operands)


def pair_kernel(place_ref, own_ref, end_ref, other_ref, rest_other_ref, _, out_ref, rest_ref):
    samples = own_ref.shape[1] // 2

    @pl.when(place_ref[1] == 1)
    def _():
        real_part, imag_part = visibility(own_ref[...], other_ref[...], samples)
        out_ref[0, 0] = real_part
        out_ref[0, 1] = imag_part
        real_part, imag_part = visibility(end_ref[...], rest_other_ref[...], samples)
        rest_ref[0] = real_part.astype(jnp.bfloat16)
        rest_ref[1] = imag_part.astype(jnp.bfloat16)


def pair_block(out, chunk, place, own, end, other, rest_other, name):
    rows, depth = own.shape
    half = rows // 2
    whole = pl.BlockSpec((rows, depth), lambda j, p: (0, 0))
    tile = pl.BlockSpec((half, depth), lambda j, p: (j, 0))
    return pl.pallas_call(
        pair_kernel,
        grid_spec=pltpu.PrefetchScalarGridSpec(
            num_scalar_prefetch=1,
            grid=(2,),
            in_specs=[whole, whole, tile, tile, pl.BlockSpec(memory_space=pl.ANY)],
            out_specs=[
                pl.BlockSpec((1, 2, rows, half), lambda j, p: (chunk, 0, 0, p[0] * 2 + j)),
                pl.BlockSpec((2, rows, half), lambda j, p: (0, 0, j)),
            ],
        ),
        out_shape=[
            jax.ShapeDtypeStruct(out.shape, out.dtype),
            jax.ShapeDtypeStruct((2, rows, rows), jnp.bfloat16),
        ],
        input_output_aliases={5: 0},
        cost_estimate=pl.CostEstimate(
            flops=8 * rows * rows * depth, bytes_accessed=8 * rows * depth + 12 * rows * rows, transcendentals=0
        ),
        name=name,
    )(place, own, end, other, rest_other, out)


def settle_kernel(chunks, rows, place_ref, *refs):
    count = len(chunks)
    rest_refs = refs[:count]
    out_ref, buf, sems = refs[count + 1:]

    @pl.when(place_ref[0] == 0)
    def _():
        copies = []
        for b in range(count):
            for part in range(2):
                buf[b, part] = rest_refs[b][part].astype(jnp.float32)
                column = pl.multiple_of(place_ref[1 + b] * rows, rows)
                copy = pltpu.make_async_copy(
                    buf.at[b, part],
                    out_ref.at[chunks[b], part, :, pl.ds(column, rows)],
                    sems.at[b, part],
                )
                copy.start()
                copies.append(copy)
        for copy in copies:
            copy.wait()


def settle(out, is_mid, items):
    chunks = [chunk for chunk, _, _ in items]
    place = jnp.stack([is_mid] + [column for _, column, _ in items]).astype(jnp.int32)
    rests = [made for _, _, made in items]
    count = len(items)
    rows = rests[0].shape[1]
    return pl.pallas_call(
        functools.partial(settle_kernel, chunks, rows),
        grid_spec=pltpu.PrefetchScalarGridSpec(
            num_scalar_prefetch=1,
            grid=(1,),
            in_specs=[pl.BlockSpec((2, rows, rows), lambda i, p: (0, 0, 0))] * count
            + [pl.BlockSpec(memory_space=pl.ANY)],
            out_specs=pl.BlockSpec(memory_space=pl.ANY),
            scratch_shapes=[
                pltpu.VMEM((count, 2, rows, rows), jnp.float32),
                pltpu.SemaphoreType.DMA((count, 2)),
            ],
        ),
        out_shape=jax.ShapeDtypeStruct(out.shape, out.dtype),
        input_output_aliases={1 + count: 0},
        cost_estimate=pl.CostEstimate(
            flops=count * 2 * rows * rows, bytes_accessed=12 * count * rows * rows, transcendentals=0
        ),
        name="settle",
    )(place, *rests, out)


def per_device_line(voltages, gains):
    channels, local_feeds, _, samples = voltages.shape
    freq_count = lax.axis_size("freq")
    feed_count = lax.axis_size("feed")
    owned = channels // freq_count
    rows = local_feeds * freq_count
    z = lax.axis_index("feed")
    is_mid = ((z == 1) | (z == 2)).astype(jnp.int32)
    low = z < 2
    near_end = jnp.where(low, 0, 3)
    near_mid = jnp.where(low, 1, 2)
    far_mid = 3 - near_mid
    far_end = 3 - near_end
    place_own = jnp.stack([z, is_mid]).astype(jnp.int32)
    place_near = jnp.stack([jnp.where(is_mid == 1, near_end, near_mid), is_mid]).astype(jnp.int32)
    place_mid = jnp.stack([far_mid, is_mid]).astype(jnp.int32)
    place_far = jnp.stack([far_end, is_mid]).astype(jnp.int32)
    gain_cols = jnp.transpose(gains, (1, 2, 0))
    out_shape = jax.ShapeDtypeStruct((owned, 2, rows, rows * feed_count), jnp.float32)
    own, near, mid, far, made = {}, {}, {}, {}, {}

    def launch(k):
        blocks = equalize(voltages, gain_cols, k, freq_count)
        arrived = lax.all_to_all(blocks, "freq", split_axis=0, concat_axis=0, tiled=True)
        own[k] = arrived.reshape(rows, 2 * samples)
        near[k] = lax.ppermute(own[k], "feed", INWARD + OUTWARD if k == 0 else INWARD)
        mid[k] = lax.ppermute(own[k], "feed", MIDDLE)
        far[k] = lax.ppermute(near[k], "feed", MIDDLE)

    def own_step(out, k):
        out = own_block(out, out_shape, k, place_own, own[k], own[k], "diag")
        return own_block(out, out_shape, k, place_near, own[k], near[k], "near") if k == 0 else out

    def near_step(out, k):
        out, rest = pair_block(out, k, place_near, own[k], near[k], near[k], own[k], "near")
        made[k, 1] = lax.ppermute(rest, "feed", OUTWARD)
        return out

    def mid_step(out, k):
        out, rest = pair_block(out, k, place_mid, own[k], near[k], mid[k], mid[k], "mid")
        made[k, 2] = lax.ppermute(rest, "feed", OUTWARD)
        return out

    def far_step(out, k):
        out, rest = pair_block(out, k, place_far, own[k], near[k], far[k], far[k], "far")
        made[k, 3] = lax.ppermute(rest, "feed", OUTWARD)
        return out

    def settle_step(out, *keys):
        columns = {1: near_mid, 2: far_mid, 3: far_end}
        return settle(out, is_mid, [(k, columns[b], made[k, b]) for k, b in keys])

    for k in range(owned):
        launch(k)
    out = own_step(None, 0)
    out = mid_step(out, 0)
    last = owned - 1
    for k in range(1, owned):
        out = own_step(out, k)
        out = near_step(out, k)
        out = mid_step(out, k)
        out = far_step(out, k - 1)
        if k >= 2:
            out = settle_step(out, *[(k - 2, b) for b in (1, 2, 3) if (k - 2, b) in made])
    out = far_step(out, last)
    if owned > 1:
        out = settle_step(out, *[(last - 1, b) for b in (1, 2, 3) if (last - 1, b) in made])
    out = settle_step(out, *[(last, b) for b in (1, 2) if (last, b) in made])
    return settle_step(out, (last, 3))


def stack_rows(own_rows, samples):
    real_part = own_rows[..., :samples]
    imag_part = own_rows[..., samples:]
    swapped = jnp.concatenate([imag_part, -real_part], axis=-1)
    return jnp.stack([own_rows, swapped], axis=1)


def per_device_gather(voltages, gains):
    channels, local_feeds, _, samples = voltages.shape
    freq_count = lax.axis_size("freq")
    owned = channels // freq_count
    gain_cols = jnp.transpose(gains, (1, 2, 0))
    results = []
    for k in range(owned):
        blocks = equalize(voltages, gain_cols, k, freq_count)
        arrived = lax.all_to_all(blocks, "freq", split_axis=0, concat_axis=0, tiled=True)
        own = arrived.reshape(freq_count * local_feeds, 2 * samples)
        columns = lax.all_gather(own, "feed", axis=0, tiled=True)
        product = jnp.einsum("qrk,fk->qrf", stack_rows(own[None], samples)[0], columns, preferred_element_type=jnp.float32)
        results.append(product * (1.0 / samples))
    return jnp.stack(results)


def solution(mesh):
    in_specs = (P(None, ("feed", "freq"), None, None), P(None, None, ("feed", "freq")))
    out_specs = P("freq", None, "feed", None)
    per_device = per_device_line if mesh.shape["feed"] == 4 else per_device_gather
    return jax.shard_map(
        per_device, mesh=mesh, in_specs=in_specs, out_specs=out_specs, check_vma=False
    )
```

```python
import functools

import jax
import jax.numpy as jnp
from jax import lax
from jax.experimental import pallas as pl
from jax.experimental.pallas import tpu as pltpu
from jax.sharding import PartitionSpec as P


CONTRACT_LAST = (((1,), (1,)), ((), ()))
INWARD = ((0, 1), (3, 2))
MIDDLE = ((1, 2), (2, 1))
OUTWARD = ((1, 0), (2, 3))
SWAPPED_CHUNKS = 2


def equalize_kernel(chunk, owned, volt_ref, gain_ref, out_ref, volt_buf, out_buf, in_sems, out_sems):
    parts, _, _, samples = volt_buf.shape
    loads = []
    for f in range(parts):
        load = pltpu.make_async_copy(volt_ref.at[f * owned + chunk], volt_buf.at[f], in_sems.at[f])
        load.start()
        loads.append(load)
    gain_real = jnp.transpose(gain_ref[0])
    gain_imag = jnp.transpose(gain_ref[1])
    stores = []
    for f in range(parts):
        c = f * owned + chunk
        real_col = gain_real[:, c:c + 1]
        imag_col = gain_imag[:, c:c + 1]
        loads[f].wait()
        volt_real = volt_buf[f, :, 0, :].astype(jnp.float32)
        volt_imag = volt_buf[f, :, 1, :].astype(jnp.float32)
        out_buf[f, :, :samples] = (real_col * volt_real - imag_col * volt_imag).astype(jnp.bfloat16)
        out_buf[f, :, samples:] = (real_col * volt_imag + imag_col * volt_real).astype(jnp.bfloat16)
        store = pltpu.make_async_copy(out_buf.at[f], out_ref.at[f], out_sems.at[f])
        store.start()
        stores.append(store)
    for store in stores:
        store.wait()


def equalize(voltages, gains, chunk, freq_count):
    channels, feeds, _, samples = voltages.shape
    shape = (freq_count, feeds, 2 * samples)
    return pl.pallas_call(
        functools.partial(equalize_kernel, chunk, channels // freq_count),
        in_specs=[pl.BlockSpec(memory_space=pl.ANY), pl.BlockSpec(memory_space=pltpu.VMEM)],
        out_specs=pl.BlockSpec(memory_space=pl.ANY),
        out_shape=jax.ShapeDtypeStruct(shape, jnp.bfloat16),
        scratch_shapes=[
            pltpu.VMEM((freq_count, feeds, 2, samples), jnp.int32),
            pltpu.VMEM(shape, jnp.bfloat16),
            pltpu.SemaphoreType.DMA((freq_count,)),
            pltpu.SemaphoreType.DMA((freq_count,)),
        ],
        cost_estimate=pl.CostEstimate(
            flops=6 * freq_count * feeds * samples * 2,
            bytes_accessed=freq_count * feeds * samples * 12,
            transcendentals=0,
        ),
        name="equalize",
    )(voltages, gains)


def visibility(left, right, samples):
    turned = jnp.concatenate([-right[:, samples:], right[:, :samples]], axis=1)
    real_part = lax.dot_general(left, right, CONTRACT_LAST, preferred_element_type=jnp.float32)
    imag_part = lax.dot_general(left, turned, CONTRACT_LAST, preferred_element_type=jnp.float32)
    return real_part * (1.0 / samples), imag_part * (1.0 / samples)


def own_kernel(place_ref, own_ref, other_ref, *refs):
    out_ref = refs[-1]
    samples = own_ref.shape[1] // 2
    real_part, imag_part = visibility(own_ref[...], other_ref[...], samples)
    out_ref[0, 0] = real_part
    out_ref[0, 1] = imag_part


def own_block(out, out_shape, chunk, place, own, other):
    rows, depth = own.shape
    half = rows // 2
    in_specs = [
        pl.BlockSpec((rows, depth), lambda j, p: (0, 0)),
        pl.BlockSpec((half, depth), lambda j, p: (j, 0)),
    ]
    operands = [own, other]
    aliases = {}
    if out is not None:
        in_specs.append(pl.BlockSpec(memory_space=pl.ANY))
        operands.append(out)
        aliases = {3: 0}
    return pl.pallas_call(
        own_kernel,
        grid_spec=pltpu.PrefetchScalarGridSpec(
            num_scalar_prefetch=1,
            grid=(2,),
            in_specs=in_specs,
            out_specs=pl.BlockSpec((1, 2, rows, half), lambda j, p: (chunk, 0, 0, p[0] * 2 + j)),
        ),
        out_shape=out_shape,
        input_output_aliases=aliases,
        cost_estimate=pl.CostEstimate(
            flops=4 * rows * rows * depth, bytes_accessed=4 * rows * depth + 8 * rows * rows, transcendentals=0
        ),
    )(place, *operands)


def pair_kernel(place_ref, own_ref, end_ref, other_ref, rest_other_ref, _, out_ref, rest_ref):
    samples = own_ref.shape[1] // 2

    @pl.when(place_ref[1] == 1)
    def _():
        real_part, imag_part = visibility(own_ref[...], other_ref[...], samples)
        out_ref[0, 0] = real_part
        out_ref[0, 1] = imag_part
        real_part, imag_part = visibility(end_ref[...], rest_other_ref[...], samples)
        rest_ref[0] = real_part.astype(jnp.bfloat16)
        rest_ref[1] = imag_part.astype(jnp.bfloat16)


def pair_block(out, chunk, place, own, end, other, rest_other):
    rows, depth = own.shape
    half = rows // 2
    whole = pl.BlockSpec((rows, depth), lambda j, p: (0, 0))
    tile = pl.BlockSpec((half, depth), lambda j, p: (j, 0))
    return pl.pallas_call(
        pair_kernel,
        grid_spec=pltpu.PrefetchScalarGridSpec(
            num_scalar_prefetch=1,
            grid=(2,),
            in_specs=[whole, whole, tile, tile, pl.BlockSpec(memory_space=pl.ANY)],
            out_specs=[
                pl.BlockSpec((1, 2, rows, half), lambda j, p: (chunk, 0, 0, p[0] * 2 + j)),
                pl.BlockSpec((2, rows, half), lambda j, p: (0, 0, j)),
            ],
        ),
        out_shape=[
            jax.ShapeDtypeStruct(out.shape, out.dtype),
            jax.ShapeDtypeStruct((2, rows, rows), jnp.bfloat16),
        ],
        input_output_aliases={5: 0},
        cost_estimate=pl.CostEstimate(
            flops=8 * rows * rows * depth, bytes_accessed=8 * rows * depth + 12 * rows * rows, transcendentals=0
        ),
    )(place, own, end, other, rest_other, out)


def settle_kernel(chunks, rows, place_ref, *refs):
    count = len(chunks)
    rest_refs = refs[:count]
    out_ref, buf, sems = refs[count + 1:]

    @pl.when(place_ref[0] == 0)
    def _():
        copies = []
        for b in range(count):
            for part in range(2):
                buf[b, part] = rest_refs[b][part].astype(jnp.float32)
                column = pl.multiple_of(place_ref[1 + b] * rows, rows)
                copy = pltpu.make_async_copy(
                    buf.at[b, part],
                    out_ref.at[chunks[b], part, :, pl.ds(column, rows)],
                    sems.at[b, part],
                )
                copy.start()
                copies.append(copy)
        for copy in copies:
            copy.wait()


def settle(out, is_mid, items):
    chunks = [chunk for chunk, _, _ in items]
    place = jnp.stack([is_mid] + [column for _, column, _ in items]).astype(jnp.int32)
    rests = [made for _, _, made in items]
    count = len(items)
    rows = rests[0].shape[1]
    return pl.pallas_call(
        functools.partial(settle_kernel, chunks, rows),
        grid_spec=pltpu.PrefetchScalarGridSpec(
            num_scalar_prefetch=1,
            grid=(1,),
            in_specs=[pl.BlockSpec((2, rows, rows), lambda i, p: (0, 0, 0))] * count
            + [pl.BlockSpec(memory_space=pl.ANY)],
            out_specs=pl.BlockSpec(memory_space=pl.ANY),
            scratch_shapes=[
                pltpu.VMEM((count, 2, rows, rows), jnp.float32),
                pltpu.SemaphoreType.DMA((count, 2)),
            ],
        ),
        out_shape=jax.ShapeDtypeStruct(out.shape, out.dtype),
        input_output_aliases={1 + count: 0},
        cost_estimate=pl.CostEstimate(
            flops=count * 2 * rows * rows, bytes_accessed=12 * count * rows * rows, transcendentals=0
        ),
        name="settle",
    )(place, *rests, out)


def per_device_line(voltages, gains):
    channels, local_feeds, _, samples = voltages.shape
    freq_count = lax.axis_size("freq")
    feed_count = lax.axis_size("feed")
    owned = channels // freq_count
    rows = local_feeds * freq_count
    z = lax.axis_index("feed")
    is_mid = ((z == 1) | (z == 2)).astype(jnp.int32)
    low = z < 2
    near_end = jnp.where(low, 0, 3)
    near_mid = jnp.where(low, 1, 2)
    far_mid = 3 - near_mid
    far_end = 3 - near_end
    place_own = jnp.stack([z, is_mid]).astype(jnp.int32)
    place_near = jnp.stack([jnp.where(is_mid == 1, near_end, near_mid), is_mid]).astype(jnp.int32)
    place_mid = jnp.stack([far_mid, is_mid]).astype(jnp.int32)
    place_far = jnp.stack([far_end, is_mid]).astype(jnp.int32)
    out_shape = jax.ShapeDtypeStruct((owned, 2, rows, rows * feed_count), jnp.float32)
    own, near, mid, far, made = {}, {}, {}, {}, {}

    def permute(value, pairs):
        return lax.ppermute(value, "feed", pairs)

    for k in range(owned):
        blocks = equalize(voltages, gains, k, freq_count)
        arrived = lax.all_to_all(blocks, "freq", split_axis=0, concat_axis=0, tiled=True)
        own[k] = arrived.reshape(rows, 2 * samples)
        near[k] = permute(own[k], INWARD + OUTWARD if k < SWAPPED_CHUNKS else INWARD)
        mid[k] = permute(own[k], MIDDLE)
        far[k] = permute(near[k], MIDDLE)

    columns = {1: near_mid, 2: far_mid, 3: far_end}
    out = None
    for step in steps(owned):
        kind, k = step[0], step[1]
        if kind == "diag":
            out = own_block(out, out_shape, k, place_own, own[k], own[k])
        elif kind == "near" and k < SWAPPED_CHUNKS:
            out = own_block(out, out_shape, k, place_near, own[k], near[k])
        elif kind == "near":
            out, rest = pair_block(out, k, place_near, own[k], near[k], near[k], own[k])
            made[k, 1] = permute(rest, OUTWARD)
        elif kind == "mid":
            out, rest = pair_block(out, k, place_mid, own[k], near[k], mid[k], mid[k])
            made[k, 2] = permute(rest, OUTWARD)
        elif kind == "end":
            out, rest = pair_block(out, k, place_far, own[k], near[k], far[k], far[k])
            made[k, 3] = permute(rest, OUTWARD)
        elif kind == "settle":
            items = [(c, columns[b], made[c, b]) for c, b in step[2] if (c, b) in made]
            out = settle(out, is_mid, items)
    return out


def steps(owned):
    order = []
    for k in range(owned + 1):
        if k < owned:
            order += [("diag", k), ("near", k), ("mid", k)]
        if k >= 1:
            if k == owned:
                order += [("settle", j, [(j, 1), (j, 2), (j, 3)]) for j in range(owned - 2)]
            order += [("end", k - 1)]
    last = owned - 1
    order += [("settle", last - 1, [(last - 1, b) for b in (1, 2, 3)])]
    order += [("settle", last, [(last, 1), (last, 2)])]
    order += [("settle", owned, [(last, 3)])]
    return order


def stack_rows(own_rows, samples):
    real_part = own_rows[..., :samples]
    imag_part = own_rows[..., samples:]
    swapped = jnp.concatenate([imag_part, -real_part], axis=-1)
    return jnp.stack([own_rows, swapped], axis=1)


def per_device_gather(voltages, gains):
    channels, local_feeds, _, samples = voltages.shape
    freq_count = lax.axis_size("freq")
    owned = channels // freq_count
    results = []
    for k in range(owned):
        blocks = equalize(voltages, gains, k, freq_count)
        arrived = lax.all_to_all(blocks, "freq", split_axis=0, concat_axis=0, tiled=True)
        own = arrived.reshape(freq_count * local_feeds, 2 * samples)
        columns = lax.all_gather(own, "feed", axis=0, tiled=True)
        product = jnp.einsum("qrk,fk->qrf", stack_rows(own[None], samples)[0], columns, preferred_element_type=jnp.float32)
        results.append(product * (1.0 / samples))
    return jnp.stack(results)


def solution(mesh):
    in_specs = (P(None, ("feed", "freq"), None, None), P(None, None, ("feed", "freq")))
    out_specs = P("freq", None, "feed", None)
    on_line = mesh.shape["feed"] == 4
    per_device = per_device_line if on_line else per_device_gather

    return jax.shard_map(per_device, mesh=mesh, in_specs=in_specs, out_specs=out_specs, check_vma=False)
```
